32 devices in a mesh: row: 4 (over z), col: 8 (over y, x, core).
Axes of the slice: x: 2, y: 2, z: 4, core: 2. Of those that a mesh axis runs over, the one named last changes fastest.
Arguments:
- right_side: float32 [16, 1024, 3072], P(None, 'row', 'col'), may hold values from -100 to 100
- cond_x: float32 [1024, 3072], P('row', 'col'), may hold values from 0.25 to 4
- cond_y: float32 [1024, 3072], P('row', 'col'), may hold values from 0.25 to 4
- pad_mask: int32 [1024, 3072], P('row', 'col'), may hold values 0 or 1
Outputs:
- solution: float32 [16, 1024, 3072], P(None, 'row', 'col')
- residual: float32 [16, 1024, 3072], P(None, 'row', 'col')
The draws below stay inside these ranges and needn't reach their ends.
All inputs are finite; a program needn't handle non-finite values. No bound on the sum of `pad_mask` on one device may be relied on, other than what follows from the above.
Results may differ from the reference program's by a relative error of at most 0.0003.
Values sent between devices are 32-bit elements; how exact they have to be, the bound alone decides.
A program may use at most 128 MiB of HBM per device.

```python
import math
import jax
import jax.numpy as jnp
from jax import lax

RHS = 16
ITERS = 3
NX = 1024
NY = 3072


def draw_right_side(key, part):
    key_rough = jax.random.fold_in(key, 11)
    key_scale = jax.random.fold_in(key, 12)
    row_pos = jnp.arange(NX, dtype=jnp.float32) / NX - 0.5
    col_pos = jnp.arange(NY, dtype=jnp.float32) / NY - 0.5
    pattern = jnp.exp(jax.random.uniform(key_scale, (RHS, 1, 1), jnp.float32, math.log(0.3), math.log(3.0)))
    roughness = jnp.clip(jax.random.normal(key_rough, (RHS, NX, NY), jnp.float32), -6.0, 6.0)
    growth = jnp.power(3.0, row_pos)[:, None] * jnp.power(3.0, col_pos)[None, :]
    return (pattern * growth[None] * roughness).astype(jnp.float32)


def place_ends(result, stream_key, low, high):
    longest = result.shape.index(max(result.shape))
    spots = []
    for shift in (0, 1):
        where = [jax.random.randint(jax.random.fold_in(stream_key, axis), (), 0, length) for axis, length in enumerate(result.shape)]
        where[longest] = (where[longest] + shift) % result.shape[longest]
        spots.append(tuple(where))
    return result.at[spots[0]].set(low).at[spots[1]].set(high)


def level_of(rng, extent, split, least, high):
    def one(dim, parts):
        steps = jax.random.uniform(jax.random.fold_in(jax.random.fold_in(rng, 6), dim), (parts,), jnp.float32, least / len(split), high / len(split))
        return jnp.repeat(jnp.exp(steps), extent[dim] // parts).reshape((-1,) + (1,) * (len(extent) - dim - 1))

    loudness = one(*split[0])
    for cut in split[1:]:
        loudness = loudness * one(*cut)
    return loudness


def setup_inputs(seed: int = 0) -> dict:
    key_of = jax.random.split(jax.random.key(seed), 5)
    right_side = draw_right_side(jax.random.fold_in(key_of[4], 71), 0)
    cond_x = jnp.clip(jnp.exp(math.log(4.0) - 2.7725887 * jax.random.uniform(key_of[1], (NX, NY), jnp.float32) ** level_of(key_of[1], (NX, NY), ((0, 4), (1, 8)), -0.2, 0.2)), 0.25, 4.0)
    cond_y = jnp.clip(jnp.exp(math.log(4.0) - 2.7725887 * jax.random.uniform(key_of[2], (NX, NY), jnp.float32) ** level_of(key_of[2], (NX, NY), ((0, 4), (1, 8)), -0.2, 0.2)), 0.25, 4.0)
    pad_mask = place_ends((jax.random.randint(key_of[3], (NX, NY), 0, 16) < 1).astype(jnp.int32), jax.random.fold_in(key_of[3], 1), 0, 1)
    return {"right_side": right_side, "cond_x": cond_x, "cond_y": cond_y, "pad_mask": pad_mask}


exact_precision = lax.Precision.HIGHEST

def neighbour_sum(padded, cond_x, cond_above, cond_y, cond_left):
    total = cond_x * padded[:, 2:, 1:-1] + cond_above * padded[:, :-2, 1:-1]
    return total + cond_y * padded[:, 1:-1, 2:] + cond_left * padded[:, 1:-1, :-2]

def gram(left, right):
    return jnp.einsum('kab,lab->kl', left, right, precision=exact_precision)

def combine(field, matrix):
    return jnp.einsum('kab,kl->lab', field, matrix, precision=exact_precision)

def small_solve(matrix, right):
    factor = jnp.linalg.cholesky(matrix)
    return jax.scipy.linalg.cho_solve((factor, True), right)

def reference(right_side, cond_x, cond_y, pad_mask):
    pad_nodes = pad_mask.astype(jnp.float32)
    free_nodes = 1.0 - pad_nodes
    cond_above = jnp.pad(cond_x, ((1, 0), (0, 0)))[:-1]
    cond_left = jnp.pad(cond_y, ((0, 0), (1, 0)))[:, :-1]
    diagonal = free_nodes * (cond_x + cond_above + cond_y + cond_left) + pad_nodes
    inverse = 1.0 / diagonal

    def operate(field):
        padded = jnp.pad(free_nodes * field, ((0, 0), (1, 1), (1, 1)))
        return pad_nodes * field + free_nodes * (diagonal * field - neighbour_sum(padded, cond_x, cond_above, cond_y, cond_left))
    solution = jnp.zeros_like(right_side)
    residual = right_side
    precond = residual * inverse
    direction = precond
    gram_now = gram(residual, precond)
    for iteration in range(ITERS):
        image = operate(direction)
        alpha_block = small_solve(gram(direction, image), gram_now)
        solution = solution + combine(direction, alpha_block)
        residual = residual - combine(image, alpha_block)
        precond = residual * inverse
        gram_next = gram(residual, precond)
        beta_block = small_solve(gram_now, gram_next)
        direction = precond + combine(direction, beta_block)
        gram_now = gram_next
    return (solution, residual)
```

```python
import functools

import jax
import jax.numpy as jnp
from jax import lax
from jax.experimental import pallas as pl
from jax.experimental.pallas import tpu as pltpu
from jax.sharding import PartitionSpec as P

ITERS = 3
F32 = jnp.float32
BF16 = jnp.bfloat16
MESH = pl.DeviceIdType.MESH
SUB = 8
LANES = 128


def exact_dot(left, right, dims):
    return lax.dot_general(
        left, right, (dims, ((), ())), precision=lax.Precision.HIGHEST, preferred_element_type=F32
    )


def fast_dot(left, right, dims):
    return lax.dot_general(left, right, (dims, ((), ())), preferred_element_type=F32)


def split(value):
    high = value.astype(BF16)
    low = (value - high.astype(F32)).astype(BF16)
    return high, low


def iota(shape, dim):
    return lax.broadcasted_iota(jnp.int32, shape, dim)


def kernel(
    nr, nc, b_ref, cx_ref, cy_ref, pad_ref, sol_ref, res_ref,
    v_ref, img_ref, ex_ref, ea_ref, ey_ref, el_ref, dg_ref, inv_ref,
    gram_ref, g0_ref,
    crow_src, crow_dst, ccol_src, ccol_dst,
    vrow_src, vrow_dst, vcol_src, vcol_dst,
    row_slots, col_slots, row_mine, col_mine,
    halo_send, halo_recv, red_send, red_recv,
):
    fields, rows, cols = b_ref.shape
    wide = fields * SUB
    tiles = rows // SUB
    pairs = tiles // 2
    row = lax.axis_index("row")
    col = lax.axis_index("col")

    barrier = pltpu.get_barrier_semaphore()
    for d in range(1, nr):
        pl.semaphore_signal(barrier, inc=1, device_id=(lax.rem(row + d, nr), col), device_id_type=MESH)
    for d in range(1, nc):
        pl.semaphore_signal(barrier, inc=1, device_id=(row, lax.rem(col + d, nc)), device_id_type=MESH)
    pl.semaphore_wait(barrier, nr - 1 + nc - 1)

    has_out = (row < nr - 1, row > 0, col < nc - 1, col > 0)
    has_in = (row > 0, row < nr - 1, col > 0, col < nc - 1)
    targets = ((row + 1, col), (row - 1, col), (row, col + 1), (row, col - 1))

    def halo_copy(stage, side, row_src, row_dst, col_src, col_dst):
        src, dst = (row_src, row_dst) if side < 2 else (col_src, col_dst)
        return pltpu.make_async_remote_copy(
            src_ref=src.at[side % 2],
            dst_ref=dst.at[side % 2],
            send_sem=halo_send.at[stage, side],
            recv_sem=halo_recv.at[stage, side],
            device_id=targets[side],
            device_id_type=MESH,
        )

    def halo_start(stage, *bufs):
        for side in range(4):
            @pl.when(has_out[side])
            def _():
                halo_copy(stage, side, *bufs).start()

    def halo_wait(stage, *bufs):
        for side in range(4):
            @pl.when(has_out[side])
            def _():
                halo_copy(stage, side, *bufs).wait_send()

            @pl.when(has_in[side])
            def _():
                halo_copy(stage, side, *bufs).wait_recv()

            dst = bufs[1] if side < 2 else bufs[3]

            @pl.when(jnp.logical_not(has_in[side]))
            def _():
                dst[side % 2] = jnp.zeros(dst.shape[1:], F32)

    lane8 = iota((SUB, LANES), 1)
    pad = pad_ref[...].astype(F32)
    free = 1.0 - pad
    cx = cx_ref[...]
    cy = cy_ref[...]

    def packed_column(array, lane):
        base = lane // LANES * LANES
        out = jnp.zeros((SUB, LANES), F32)
        for r in range(tiles):
            tile = array[r * SUB:(r + 1) * SUB, base:base + LANES]
            out = jnp.where(lane8 == r, pltpu.roll(tile, (r - lane) % LANES, 1), out)
        return out

    def unpacked_column(packed, lane):
        return jnp.concatenate(
            [pltpu.roll(packed, (lane - r) % LANES, 1) for r in range(tiles)], axis=0
        )

    crow_src[0, 0:1, :] = cx[rows - 1:rows]
    crow_src[0, 1:2, :] = free[rows - 1:rows]
    crow_src[0, 2:SUB, :] = jnp.zeros((SUB - 2, cols), F32)
    crow_src[1] = jnp.broadcast_to(free[0:1], (SUB, cols))
    ccol_src[0, 0:SUB] = packed_column(cy, cols - 1)
    ccol_src[0, SUB:] = packed_column(free, cols - 1)
    first = packed_column(free, 0)
    ccol_src[1, 0:SUB] = first
    ccol_src[1, SUB:] = first
    cond_bufs = (crow_src, crow_dst, ccol_src, ccol_dst)
    halo_start(0, *cond_bufs)
    halo_wait(0, *cond_bufs)

    rowi = iota((rows, cols), 0)
    lane = iota((rows, LANES), 1)

    def from_above(array, halo):
        return jnp.where(rowi == 0, halo, pltpu.roll(array, 1, 0))

    def from_below(array, halo):
        return jnp.where(rowi == rows - 1, halo, pltpu.roll(array, rows - 1, 0))

    def from_left(array, halo):
        rolled = pltpu.roll(array, 1, 1)
        edge = jnp.where(lane == 0, halo, rolled[:, :LANES])
        return edge if cols == LANES else jnp.concatenate([edge, rolled[:, LANES:]], axis=1)

    def from_right(array, halo):
        rolled = pltpu.roll(array, cols - 1, 1)
        edge = jnp.where(lane == LANES - 1, halo, rolled[:, cols - LANES:])
        return edge if cols == LANES else jnp.concatenate([rolled[:, :cols - LANES], edge], axis=1)

    cx_up = crow_dst[0, 0:1, :]
    cond_above = from_above(cx, cx_up)
    cond_left = from_left(cy, unpacked_column(ccol_dst[0, 0:SUB], 0))
    diagonal = free * (cx + cond_above + cy + cond_left) + pad
    dg_ref[...] = diagonal
    inv_ref[...] = 1.0 / diagonal
    ex_ref[...] = free * cx * from_below(free, crow_dst[1, 0:1, :])
    ea_ref[...] = free * cond_above * from_above(free, crow_dst[0, 1:2, :])
    ey_ref[...] = free * cy * from_right(free, unpacked_column(ccol_dst[1, 0:SUB], LANES - 1))
    el_ref[...] = free * cond_left * from_left(free, unpacked_column(ccol_dst[0, SUB:], 0))

    lane_w = iota((wide, LANES), 1)
    lane3 = iota((fields, SUB, LANES), 2)
    sub3 = iota((fields, SUB, cols), 1)

    def rows_at(r):
        return pl.ds(pl.multiple_of(r * SUB, SUB), SUB)

    def store_direction(stage, r, value):
        v_ref[:, rows_at(r + 1), :] = value.reshape(fields, SUB, cols)
        right = pltpu.roll(value[:, cols - LANES:], lax.rem(r + 1, LANES), 1)
        left = pltpu.roll(value[:, :LANES], lax.rem(r + LANES, LANES), 1)
        hit = lane_w == r
        vcol_src[stage, 0] = jnp.where(hit, right, vcol_src[stage, 0])
        vcol_src[stage, 1] = jnp.where(hit, left, vcol_src[stage, 1])

    def direction_bufs(stage):
        return (vrow_src.at[stage], vrow_dst.at[stage], vcol_src.at[stage], vcol_dst.at[stage])

    def direction_start(stage):
        vrow_src[stage, 0] = v_ref[:, rows:rows + SUB, :][:, SUB - 1, :]
        vrow_src[stage, 1] = v_ref[:, SUB:2 * SUB, :][:, 0, :]
        halo_start(stage + 1, *direction_bufs(stage))

    def direction_wait(stage):
        halo_wait(stage + 1, *direction_bufs(stage))
        top = vrow_dst[stage, 0]
        bottom = vrow_dst[stage, 1]
        v_ref[:, 0:SUB, :] = jnp.broadcast_to(top[:, None, :], (fields, SUB, cols))
        v_ref[:, rows + SUB:, :] = jnp.broadcast_to(bottom[:, None, :], (fields, SUB, cols))

    def operate(stage, r):
        cur = v_ref[:, rows_at(r + 1), :]
        prev = v_ref[:, rows_at(r), :]
        after = v_ref[:, rows_at(r + 2), :]
        up = pltpu.roll(jnp.where(sub3 == SUB - 1, prev, cur), 1, 1)
        down = pltpu.roll(jnp.where(sub3 == 0, after, cur), SUB - 1, 1)
        left = pltpu.roll(cur, 1, 2)
        right = pltpu.roll(cur, cols - 1, 2)
        halo_left = pltpu.roll(vcol_dst[stage, 0], lax.rem(LANES - r, LANES), 1)
        halo_right = pltpu.roll(vcol_dst[stage, 1], LANES - 1 - r, 1)
        edge_left = jnp.where(lane3 == 0, halo_left.reshape(fields, SUB, LANES), left[:, :, :LANES])
        edge_right = jnp.where(
            lane3 == LANES - 1, halo_right.reshape(fields, SUB, LANES), right[:, :, cols - LANES:]
        )
        if cols > LANES:
            edge_left = jnp.concatenate([edge_left, left[:, :, LANES:]], axis=2)
            edge_right = jnp.concatenate([right[:, :, :cols - LANES], edge_right], axis=2)
        at = rows_at(r)
        image = (
            dg_ref[at, :][None] * cur
            - (ex_ref[at, :][None] * down + ea_ref[at, :][None] * up)
            - (ey_ref[at, :][None] * edge_right + el_ref[at, :][None] * edge_left)
        )
        img_ref[:, at, :] = image
        return image

    def flat(value):
        return value.reshape(wide, cols)

    def gram_step(left, rights):
        lh, ll = split(left)
        highs, lows = zip(*[split(right) for right in rights])
        rh = jnp.concatenate(highs, axis=0) if len(highs) > 1 else highs[0]
        rl = jnp.concatenate(lows, axis=0) if len(lows) > 1 else lows[0]
        return fast_dot(
            jnp.concatenate([lh, lh, ll], axis=1), jnp.concatenate([rh, rl, rh], axis=1), ((1,), (1,))
        )

    def begin(r, carry):
        at = rows_at(r)
        store_direction(0, r, flat(b_ref[:, at, :] * inv_ref[at, :][None]))
        return carry

    for stage in range(ITERS):
        for side in range(2):
            vcol_src[stage, side] = jnp.zeros((wide, LANES), F32)
    lax.fori_loop(0, tiles, begin, 0)
    direction_start(0)

    g0_ref[...] = jnp.zeros((wide, wide), F32)

    def first_gram(p, carry):
        lefts = [flat(b_ref[:, rows_at(2 * p + h), :]) for h in range(2)]
        rights = [flat(v_ref[:, rows_at(2 * p + h + 1), :]) for h in range(2)]
        g0_ref[...] += gram_step(jnp.concatenate(lefts, axis=1), [jnp.concatenate(rights, axis=1)])
        return carry

    lax.fori_loop(0, pairs, first_gram, 0)

    pick = (iota((fields, wide), 1) // SUB == iota((fields, wide), 0)).astype(F32)
    same = lax.rem(iota((wide, wide), 0), SUB) == lax.rem(iota((wide, wide), 1), SUB)

    def reduced(block):
        part = exact_dot(pick, jnp.where(same, block, 0.0), ((1,), (0,)))
        return exact_dot(part, pick, ((1,), (1,)))

    def all_sum(stage, value):
        for phase, (count, me, slots, mine) in enumerate(
            ((nr, row, row_slots, row_mine), (nc, col, col_slots, col_mine))
        ):
            mine[stage] = value
            slots[stage, me] = value
            copies = []
            for d in range(1, count):
                peer = lax.rem(me + d, count)
                copies.append(
                    pltpu.make_async_remote_copy(
                        src_ref=mine.at[stage],
                        dst_ref=slots.at[stage, me],
                        send_sem=red_send.at[stage, phase, d],
                        recv_sem=red_recv.at[stage, phase, d],
                        device_id=(peer, col) if phase == 0 else (row, peer),
                        device_id_type=MESH,
                    )
                )
            for copy in copies:
                copy.start()
            for copy in copies:
                copy.wait()
            value = slots[stage, 0]
            for d in range(1, count):
                value = value + slots[stage, d]
        return value

    def kron(matrix):
        half = exact_dot(matrix, pick, ((0,), (0,)))
        full = exact_dot(pick, half, ((0,), (0,)))
        high, low = split(jnp.where(same, full, 0.0))
        return jnp.concatenate([high, high], axis=1), jnp.concatenate([low, low], axis=1)

    def combined(coefs, value):
        high, low = split(value)
        both = jnp.concatenate([high, low], axis=0)
        return [
            fast_dot(h, both, ((1,), (0,))) + fast_dot(l, both, ((1,), (0,))) for h, l in coefs
        ]

    rowf = iota((fields, LANES), 0)

    def padded(parts):
        spare = jnp.zeros((fields, LANES - fields * len(parts)), F32)
        return jnp.concatenate(list(parts) + [spare], axis=1)

    gram_now = None
    for step in range(ITERS):
        last = step == ITERS - 1
        direction_wait(step)
        terms = 1 if last else (2 if step == 0 else 3)
        span = terms * wide
        gram_ref[:, 0:span] = jnp.zeros((wide, span), F32)

        def stencil(p, carry, step=step, terms=terms, span=span):
            images, groups = [], [[] for _ in range(terms)]
            for h in range(2):
                r = 2 * p + h
                at = rows_at(r)
                image = operate(step, r)
                images.append(flat(image))
                groups[0].append(flat(v_ref[:, rows_at(r + 1), :]))
                if terms > 1:
                    groups[1].append(flat(image * inv_ref[at, :][None]))
                if terms > 2:
                    groups[2].append(flat(res_ref[:, at, :] * inv_ref[at, :][None]))
            gram_ref[:, 0:span] += gram_step(
                jnp.concatenate(images, axis=1), [jnp.concatenate(g, axis=1) for g in groups]
            )
            return carry

        lax.fori_loop(0, pairs, stencil, 0)
        parts = [reduced(gram_ref[:, t * wide:(t + 1) * wide]) for t in range(terms)]
        if step == 0:
            parts.append(reduced(g0_ref[...]))
        total = all_sum(step, padded(parts))
        curvature = total[:, 0:fields]
        if step == 0:
            gram_now = total[:, 2 * fields:3 * fields]
        system = padded([curvature, gram_now])
        unit = (iota((fields, fields), 0) == iota((fields, fields), 1)).astype(F32)
        other = padded([gram_now, unit])
        for j in range(fields):
            scaled = system[j:j + 1, :] / system[j:j + 1, j:j + 1]
            system = jnp.where(rowf == j, scaled, system - system[:, j:j + 1] * scaled)
            if not last:
                scaled = other[j:j + 1, :] / other[j:j + 1, j:j + 1]
                other = jnp.where(rowf == j, scaled, other - other[:, j:j + 1] * scaled)
        alpha = system[:, fields:2 * fields]
        coefs = [kron(alpha)]
        if not last:
            image_term = total[:, fields:2 * fields]
            cross = curvature if step == 0 else total[:, 2 * fields:3 * fields]
            mixed = exact_dot(alpha, cross, ((0,), (0,)))
            mixed_t = exact_dot(cross, alpha, ((0,), (0,)))
            quadratic = exact_dot(
                exact_dot(alpha, image_term, ((0,), (0,))), alpha, ((1,), (0,))
            )
            gram_next = gram_now - mixed - mixed_t + quadratic
            beta = exact_dot(other[:, fields:2 * fields], gram_next, ((1,), (0,)))
            coefs.append(kron(beta))
            gram_now = gram_next

        def update(p, carry, step=step, last=last, coefs=coefs):
            v = jnp.concatenate([flat(v_ref[:, rows_at(2 * p + h + 1), :]) for h in range(2)], axis=1)
            image = jnp.concatenate([flat(img_ref[:, rows_at(2 * p + h), :]) for h in range(2)], axis=1)
            moved = combined(coefs, v)
            drop = combined(coefs[:1], image)[0]
            for h in range(2):
                r = 2 * p + h
                at = rows_at(r)
                part = slice(h * cols, (h + 1) * cols)
                shift = moved[0][:, part].reshape(fields, SUB, cols)
                if step == 0:
                    sol_ref[:, at, :] = shift
                    old = b_ref[:, at, :]
                else:
                    sol_ref[:, at, :] += shift
                    old = res_ref[:, at, :]
                residual = old - drop[:, part].reshape(fields, SUB, cols)
                res_ref[:, at, :] = residual
                if not last:
                    store_direction(
                        step + 1, r, flat(residual * inv_ref[at, :][None]) + moved[1][:, part]
                    )
            return carry

        lax.fori_loop(0, pairs, update, 0)
        if not last:
            direction_start(step + 1)


def shards(right_side, cond_x, cond_y, pad_mask):
    fields, rows, cols = right_side.shape
    nr = lax.axis_size("row")
    nc = lax.axis_size("col")
    wide = fields * SUB
    vmem = lambda *shape: pltpu.VMEM(shape, F32)
    plane = vmem(rows, cols)
    out = jax.ShapeDtypeStruct(right_side.shape, F32)
    return pl.pallas_call(
        functools.partial(kernel, nr, nc),
        out_shape=(out, out),
        in_specs=[pl.BlockSpec(memory_space=pltpu.VMEM)] * 4,
        out_specs=(pl.BlockSpec(memory_space=pltpu.VMEM),) * 2,
        scratch_shapes=[
            vmem(fields, rows + 2 * SUB, cols),
            vmem(fields, rows, cols),
            plane, plane, plane, plane, plane, plane,
            vmem(wide, 3 * wide), vmem(wide, wide),
            vmem(2, SUB, cols), vmem(2, SUB, cols),
            vmem(2, 2 * SUB, LANES), vmem(2, 2 * SUB, LANES),
            vmem(ITERS, 2, fields, cols), vmem(ITERS, 2, fields, cols),
            vmem(ITERS, 2, wide, LANES), vmem(ITERS, 2, wide, LANES),
            vmem(ITERS, nr, fields, LANES), vmem(ITERS, nc, fields, LANES),
            vmem(ITERS, fields, LANES), vmem(ITERS, fields, LANES),
            pltpu.SemaphoreType.DMA((ITERS + 1, 4)), pltpu.SemaphoreType.DMA((ITERS + 1, 4)),
            pltpu.SemaphoreType.DMA((ITERS, 2, max(nr, nc))),
            pltpu.SemaphoreType.DMA((ITERS, 2, max(nr, nc))),
        ],
        compiler_params=pltpu.CompilerParams(
            collective_id=0, has_side_effects=True, vmem_limit_bytes=60 * 1024 * 1024
        ),
        name="block_cg",
    )(right_side, cond_x, cond_y, pad_mask)


def solution(mesh):
    in_specs = (P(None, "row", "col"), P("row", "col"), P("row", "col"), P("row", "col"))
    out_specs = (P(None, "row", "col"), P(None, "row", "col"))
    return jax.shard_map(shards, mesh=mesh, in_specs=in_specs, out_specs=out_specs, check_vma=False)
```
